32 devices in a mesh: ctx: 8 (over z, core), tp: 4 (over y, x).
Axes of the slice: x: 2, y: 2, z: 4, core: 2. Of those that a mesh axis runs over, the one named last changes fastest.
Arguments:
- act_codes: bfloat16 [2048, 4096], P(('ctx', 'tp')), may hold values from -6 to 6
- scale_exps: int32 [2048, 32], P(('ctx', 'tp')), may hold values from -2 to 2
- weight: bfloat16 [4096, 6144], P(None, 'tp'), may hold values from -0.09375 to 0.09375
- grad_out: bfloat16 [2048, 6144], P('ctx', 'tp'), may hold values from -6 to 6
Outputs:
- grad_input: bfloat16 [2048, 4096], P(('ctx', 'tp'))
- grad_weight: float32 [4096, 6144], P('ctx', 'tp')
The draws below stay inside these ranges and needn't reach their ends.
All inputs are finite; a program needn't handle non-finite values.
Results may differ from the reference program's by a relative error of at most 0.023.
Values may be sent and summed in bfloat16 or wider, within the bound.
A program may use at most 64 MiB of HBM per device.

```python
import jax
import jax.numpy as jnp
from jax import lax

D = 4096
BLOCK = 128
QKVW = 6144
TOKENS = 2048
N_TP = 4


def plant(array, own_key, least, high):
    place = [jax.random.randint(jax.random.fold_in(own_key, axis), (), 0, length) for axis, length in enumerate(array.shape)]
    longest = array.shape.index(max(array.shape))
    neighbour = place[:longest] + [(place[longest] + 1) % array.shape[longest]] + place[longest + 1:]
    return array.at[tuple(place)].set(least).at[tuple(neighbour)].set(high)


def strengthened(array, own_key, source, target, parts, factor):
    owner, partner = [(jnp.arange(array.shape[axis_at]) // (array.shape[axis_at] // parts)).reshape([-1 if axis == axis_at else 1 for axis in range(array.ndim)]) for axis_at in (source, target)]
    chosen = jax.random.permutation(own_key, parts)[partner]
    strong = (owner == chosen) | (owner == (partner + parts // 2) % parts)
    return jnp.where(strong, factor * array, array)


def levels(stream_key, shape, shards, low, top_value):
    loudness, own = 1.0, jax.random.fold_in(stream_key, 6)
    for position, parts in shards:
        steps = jnp.exp(jax.random.uniform(jax.random.fold_in(own, position), (parts,), jnp.float32, low / len(shards), top_value / len(shards)))
        loudness = loudness * jnp.repeat(steps, shape[position] // parts).reshape([-1 if axis == position else 1 for axis in range(len(shape))])
    return loudness


def gaussian(own_key, dims, deviation, reach, cuts=(), kind=jnp.bfloat16):
    values = jax.random.normal(own_key, dims, jnp.float32) * deviation
    if len(cuts) > 0:
        values = levels(own_key, dims, cuts, -0.22, 0.18) * values
    return jnp.clip(values, min=-reach, max=reach).astype(kind)


def noise_with(stream_key, extent, scale, reach, pieces, heavy, held_as=jnp.bfloat16):
    drawn = scale * jax.random.normal(stream_key, extent, jnp.float32)
    if pieces:
        drawn = drawn * levels(stream_key, extent, pieces, -0.22, 0.18)
    return jnp.clip(strengthened(drawn, jax.random.fold_in(stream_key, 3), *heavy), -reach, reach).astype(held_as)


def setup_inputs(seed: int = 0) -> dict:
    key_list = jax.random.split(jax.random.key(seed), 5)
    act_codes = noise_with(key_list[0], (TOKENS, D), 1.0, 6.0, ((0, 32),), (0, 1, 32, 2.75))
    scale_exps = plant(jax.random.randint(key_list[1], (TOKENS, D // BLOCK), -2, 3), jax.random.fold_in(key_list[1], 1), -2, 2).astype(jnp.int32)
    weight = gaussian(key_list[2], (D, QKVW), D ** -0.5, 0.09375, ((1, 4),))
    grad_out = noise_with(key_list[3], (TOKENS, QKVW), 1.0, 6.0, ((0, 8), (1, 4)), (1, 0, 8, 2.0))
    return {"act_codes": act_codes, "scale_exps": scale_exps, "weight": weight, "grad_out": grad_out}


def dequantize(act_codes, scale_exps):
    tok_rows = act_codes.shape[0]
    scales = jnp.exp2(scale_exps.astype(jnp.float32))
    blocked = act_codes.astype(jnp.float32).reshape(tok_rows, D // BLOCK, BLOCK) * scales[:, :, None]
    return blocked.reshape(tok_rows, D).astype(jnp.bfloat16)

def reference(act_codes, scale_exps, weight, grad_out):
    acts = dequantize(act_codes, scale_exps)
    grad_weight = jnp.dot(acts.T, grad_out, preferred_element_type=jnp.float32)
    grad_weight = grad_weight * lax.rsqrt(jnp.float32(TOKENS))
    width = QKVW // N_TP

    def add_block(total, index):
        offset = (index * width).astype(jnp.int32)
        grads = lax.dynamic_slice_in_dim(grad_out, offset, width, 1)
        weights = lax.dynamic_slice_in_dim(weight, offset, width, 1)
        part = lax.dot_general(grads, weights, (((1,), (1,)), ((), ())), preferred_element_type=jnp.float32)
        part = lax.optimization_barrier(part.astype(jnp.bfloat16))
        return (total + part.astype(jnp.float32), None)
    total, unused = lax.scan(add_block, jnp.zeros((TOKENS, D), jnp.float32), jnp.arange(N_TP, dtype=jnp.int32))
    return (total.astype(jnp.bfloat16), grad_weight)
```

```python
import functools

import jax
import jax.numpy as jnp
from jax import lax
from jax.experimental import pallas as pl
from jax.experimental.pallas import tpu as pltpu
from jax.sharding import PartitionSpec as P

MESH = pl.DeviceIdType.MESH
CHUNKS = 2


def kernel(
    n_ctx, n_tp, tokens,
    codes_ref, exps_ref, weight_ref, grads_ref,
    gin_ref, gw_ref,
    w_buf, g_buf, a_send, a_buf, part, landed,
    w_sem, g_sem,
    a_ssem, a_rsem, b_ssem, b_rsem, up_ssem, down_ssem, mate_ssem, g_rsem, p_ssem, p_rsem,
):
    n_line = n_ctx // 2
    me = lax.axis_index("ctx")
    tp = lax.axis_index("tp")
    core = lax.rem(me, 2)
    z = lax.div(me, 2)
    mate = me + 1 - 2 * core
    rows, width = codes_ref.shape
    block = width // exps_ref.shape[1]
    feats = width // n_ctx
    d_tile = w_buf.shape[1]
    n_d = w_buf.shape[0]
    scale = lax.rsqrt(jnp.float32(tokens))
    split = n_ctx * n_tp <= 64

    def load_w(i):
        return pltpu.make_async_copy(
            weight_ref.at[pl.ds(i * d_tile, d_tile)], w_buf.at[i], w_sem.at[i]
        )

    def load_g(k):
        size = g_buf.shape[2]
        return pltpu.make_async_copy(
            grads_ref.at[pl.ds(k * size, size)], g_buf.at[me, k], g_sem.at[k]
        )

    for k in range(CHUNKS):
        load_g(k).start()
    for i in range(n_d):
        load_w(i).start()

    barrier = pltpu.get_barrier_semaphore()
    for r in range(1, n_ctx):
        pl.semaphore_signal(
            barrier, inc=1, device_id=(lax.rem(me + r, n_ctx), tp), device_id_type=MESH
        )
    for r in range(1, n_tp):
        pl.semaphore_signal(
            barrier, inc=1, device_id=(me, lax.rem(tp + r, n_tp)), device_id_type=MESH
        )

    for b in range(width // block):
        owner, place = divmod(b * block, feats)
        power = jnp.exp2(exps_ref[:, b : b + 1].astype(jnp.float32))
        value = codes_ref[:, b * block : (b + 1) * block].astype(jnp.float32) * power
        a_send[owner, :, place : place + block] = value.astype(jnp.bfloat16)

    pl.semaphore_wait(barrier, n_ctx + n_tp - 2)

    def remote(src, dst, ssem, rsem, to):
        return pltpu.make_async_remote_copy(
            src_ref=src, dst_ref=dst, send_sem=ssem, recv_sem=rsem,
            device_id=to, device_id_type=MESH,
        )

    def act_copy(to):
        return remote(
            a_send.at[to], a_buf.at[me, tp], a_ssem.at[to], a_rsem.at[me], (to, tp)
        )

    def act_landing(source):
        return remote(
            a_send.at[source], a_buf.at[source, tp], a_ssem.at[source], a_rsem.at[source],
            (source, tp),
        )

    def spread_copy(s, q, src=None):
        return remote(
            a_buf.at[s, tp] if src is None else src,
            a_buf.at[s, tp], b_ssem.at[s, q], b_rsem.at[s, tp], (me, q),
        )

    def spread_landing(s, q):
        return remote(
            a_buf.at[s, q], a_buf.at[s, q], b_ssem.at[s, q], b_rsem.at[s, q], (me, q)
        )

    def spread_all(q):
        return remote(
            a_buf.at[:, tp], a_buf.at[:, tp], b_ssem.at[0, q], b_rsem.at[0, tp], (me, q)
        )

    def spread_all_landing(q):
        return remote(
            a_buf.at[:, q], a_buf.at[:, q], b_ssem.at[0, q], b_rsem.at[0, q], (me, q)
        )

    def pass_on(s, k, ssem, to):
        return remote(
            g_buf.at[s, k], g_buf.at[s, k], ssem.at[lax.div(s, 2), k], g_rsem.at[s, k], (to, tp)
        )

    def up(s, k):
        return pass_on(s, k, up_ssem, me + 2)

    def down(s, k):
        return pass_on(s, k, down_ssem, me - 2)

    def across(s, k):
        return pass_on(s, k, mate_ssem, mate)

    has_up = z < n_line - 1
    has_down = z > 0

    for r in range(1, n_ctx):
        act_copy(lax.rem(me + r, n_ctx)).start()
    for k in range(CHUNKS):
        load_g(k).wait()

        @pl.when(has_up)
        def _():
            up(me, k).start()

        @pl.when(has_down)
        def _():
            down(me, k).start()

        across(me, k).start()

    peers = [lax.rem(tp + r, n_tp) for r in range(1, n_tp)]
    if split:
        for q in peers:
            spread_copy(me, q, a_send.at[me]).start()
    a_buf[me, tp] = a_send[me]
    for r in range(1, n_ctx):
        s = lax.rem(me + r, n_ctx)
        act_landing(s).wait_recv()
        if split:
            for q in peers:
                spread_copy(s, q).start()
    if not split:
        for q in peers:
            spread_all(q).start()

    grads = g_buf[me].reshape(-1, g_buf.shape[3])
    for i in range(n_d):
        load_w(i).wait()
        piece = lax.dot_general(
            grads, w_buf[i], (((1,), (1,)), ((), ())), preferred_element_type=jnp.float32
        ).astype(jnp.bfloat16)
        part[:, :, i * d_tile : (i + 1) * d_tile] = piece.reshape(n_tp, rows, d_tile)

    def part_copy(q):
        return remote(part.at[q], landed.at[tp], p_ssem.at[q], p_rsem.at[tp], (me, q))

    def part_landing(q):
        return remote(part.at[q], landed.at[q], p_ssem.at[q], p_rsem.at[q], (me, q))

    for q in peers:
        part_copy(q).start()

    n_cols = g_buf.shape[3]
    n_tile = 512 if n_cols % 512 == 0 else n_cols

    def accumulate(zz, first):
        lhs = a_buf[pl.ds(2 * zz, 2)].reshape(-1, feats).T

        for j in range(n_cols // n_tile):
            cols = slice(j * n_tile, (j + 1) * n_tile)
            rhs = g_buf[pl.ds(2 * zz, 2), :, :, cols].reshape(-1, n_tile)
            term = jnp.dot(lhs, rhs, preferred_element_type=jnp.float32) * scale
            if first:
                gw_ref[:, cols] = term
            else:
                gw_ref[:, cols] += term

    def chip_terms(zz, first=False):
        other = 2 * zz + 1 - core
        for k in range(CHUNKS):
            across(other, k).wait_recv()
        if split:
            for c in range(2):
                for q in peers:
                    spread_landing(2 * zz + c, q).wait_recv()
        elif first:
            for q in peers:
                spread_all_landing(q).wait_recv()
        accumulate(zz, first)

    def terms_at(d):
        if d == 0:
            chip_terms(z, True)
            return

        @pl.when(z >= d)
        def _():
            chip_terms(z - d)

        @pl.when(z + d < n_line)
        def _():
            chip_terms(z + d)

    def sum_parts():
        for q in peers:
            part_landing(q).wait_recv()
        total = part[tp].astype(jnp.float32)
        for q in peers:
            total = total + landed[q].astype(jnp.float32)
        gin_ref[...] = total.astype(jnp.bfloat16)

    for d in range(1, n_line):
        if d == n_line - 1:
            sum_parts()
        for k in range(CHUNKS):

            @pl.when(z >= d)
            def _():
                s = me - 2 * d
                up(s, k).wait_recv()

                @pl.when(has_up)
                def _():
                    up(s, k).start()

                across(s, k).start()

            @pl.when(z + d < n_line)
            def _():
                s = me + 2 * d
                down(s, k).wait_recv()

                @pl.when(has_down)
                def _():
                    down(s, k).start()

                across(s, k).start()

        terms_at(d - 1)
    terms_at(n_line - 1)

    for r in range(1, n_ctx):
        act_copy(lax.rem(me + r, n_ctx)).wait_send()
    for q in peers:
        part_copy(q).wait_send()
        if split:
            for s in range(n_ctx):
                spread_copy(s, q).wait_send()
        else:
            spread_all(q).wait_send()
    for zz in range(n_line):
        for k in range(CHUNKS):
            s = 2 * zz + core
            across(s, k).wait_send()

            @pl.when(has_up & (zz <= z))
            def _():
                up(s, k).wait_send()

            @pl.when(has_down & (zz >= z))
            def _():
                down(s, k).wait_send()


def body(act_codes, scale_exps, weight, grad_out):
    n_ctx, n_tp = lax.axis_size("ctx"), lax.axis_size("tp")
    n_line = n_ctx // 2
    rows, width = act_codes.shape
    toks, cols = grad_out.shape
    feats = width // n_ctx
    d_tile = min(512, width)
    dma = pltpu.SemaphoreType.DMA
    vmem = pl.BlockSpec(memory_space=pltpu.VMEM)
    hbm = pl.BlockSpec(memory_space=pl.ANY)
    bf16 = jnp.bfloat16
    return pl.pallas_call(
        functools.partial(kernel, n_ctx, n_tp, toks * n_ctx),
        out_shape=(
            jax.ShapeDtypeStruct((rows, width), bf16),
            jax.ShapeDtypeStruct((feats, cols), jnp.float32),
        ),
        in_specs=[vmem, vmem, hbm, hbm],
        out_specs=(vmem, vmem),
        scratch_shapes=[
            pltpu.VMEM((width // d_tile, d_tile, cols), bf16),
            pltpu.VMEM((n_ctx, CHUNKS, toks // CHUNKS, cols), bf16),
            pltpu.VMEM((n_ctx, rows, feats), bf16),
            pltpu.VMEM((n_ctx, n_tp, rows, feats), bf16),
            pltpu.VMEM((n_tp, rows, width), bf16),
            pltpu.VMEM((n_tp, rows, width), bf16),
            dma((width // d_tile,)),
            dma((CHUNKS,)),
            dma((n_ctx,)),
            dma((n_ctx,)),
            dma((n_ctx if n_ctx * n_tp <= 64 else 1, n_tp)),
            dma((n_ctx if n_ctx * n_tp <= 64 else 1, n_tp)),
            dma((n_line, CHUNKS)),
            dma((n_line, CHUNKS)),
            dma((n_line, CHUNKS)),
            dma((n_ctx, CHUNKS)),
            dma((n_tp,)),
            dma((n_tp,)),
        ],
        compiler_params=pltpu.CompilerParams(
            collective_id=0, has_side_effects=True, vmem_limit_bytes=60 * 1024 * 1024
        ),
    )(act_codes, scale_exps, weight, grad_out)


def solution(mesh):
    placed = (P(("ctx", "tp"), None), P(("ctx", "tp"), None), P(None, "tp"), P("ctx", "tp"))
    return jax.shard_map(
        body,
        mesh=mesh,
        in_specs=placed,
        out_specs=(P(("ctx", "tp"), None), P("ctx", "tp")),
        check_vma=False,
    )
```

```python
import functools

import jax
import jax.numpy as jnp
from jax import lax
from jax.experimental import pallas as pl
from jax.experimental.pallas import tpu as pltpu
from jax.sharding import PartitionSpec as P

MESH = pl.DeviceIdType.MESH
CHUNKS = 4


def kernel(
    n_ctx, n_tp, tokens,
    codes_hbm, exps_hbm, weight_ref, grads_ref,
    gin_ref, gw_ref,
    codes_ref, exps_ref, w_buf, g_buf, a_send, a_buf, part, landed,
    in_sem, w_sem, g_sem,
    a_ssem, a_rsem, b_ssem, b_rsem, up_ssem, down_ssem, mate_ssem, g_rsem, p_ssem, p_rsem,
):
    n_line = n_ctx // 2
    me = lax.axis_index("ctx")
    tp = lax.axis_index("tp")
    core = lax.rem(me, 2)
    z = lax.div(me, 2)
    mate = me + 1 - 2 * core
    rows, width = codes_ref.shape
    block = width // exps_ref.shape[0]
    feats = width // n_ctx
    d_tile = w_buf.shape[1]
    n_d = w_buf.shape[0]
    scale = lax.rsqrt(jnp.float32(tokens))
    split = n_ctx * n_tp <= 64

    def load_w(i):
        return pltpu.make_async_copy(
            weight_ref.at[pl.ds(i * d_tile, d_tile)], w_buf.at[i], w_sem.at[i]
        )

    def load_g(k):
        size = g_buf.shape[2]
        return pltpu.make_async_copy(
            grads_ref.at[pl.ds(k * size, size)], g_buf.at[me, k], g_sem.at[k]
        )

    load_codes = pltpu.make_async_copy(codes_hbm, codes_ref, in_sem.at[0])
    load_exps = pltpu.make_async_copy(exps_hbm, exps_ref, in_sem.at[1])
    load_g(0).start()
    load_codes.start()
    load_exps.start()
    for k in range(1, CHUNKS):
        load_g(k).start()
    for i in range(n_d):
        load_w(i).start()

    barrier = pltpu.get_barrier_semaphore()
    for r in range(1, n_ctx):
        pl.semaphore_signal(
            barrier, inc=1, device_id=(lax.rem(me + r, n_ctx), tp), device_id_type=MESH
        )
    for r in range(1, n_tp):
        pl.semaphore_signal(
            barrier, inc=1, device_id=(me, lax.rem(tp + r, n_tp)), device_id_type=MESH
        )

    pl.semaphore_wait(barrier, n_ctx + n_tp - 2)

    def remote(src, dst, ssem, rsem, to):
        return pltpu.make_async_remote_copy(
            src_ref=src, dst_ref=dst, send_sem=ssem, recv_sem=rsem,
            device_id=to, device_id_type=MESH,
        )

    def act_copy(to):
        return remote(
            a_send.at[to], a_buf.at[me, tp], a_ssem.at[to], a_rsem.at[me], (to, tp)
        )

    def act_landing(source):
        return remote(
            a_send.at[source], a_buf.at[source, tp], a_ssem.at[source], a_rsem.at[source],
            (source, tp),
        )

    def spread_copy(s, q, src=None):
        return remote(
            a_buf.at[s, tp] if src is None else src,
            a_buf.at[s, tp], b_ssem.at[s, q], b_rsem.at[s, tp], (me, q),
        )

    def spread_landing(s, q):
        return remote(
            a_buf.at[s, q], a_buf.at[s, q], b_ssem.at[s, q], b_rsem.at[s, q], (me, q)
        )

    def spread_all(q):
        return remote(
            a_buf.at[:, tp], a_buf.at[:, tp], b_ssem.at[0, q], b_rsem.at[0, tp], (me, q)
        )

    def spread_all_landing(q):
        return remote(
            a_buf.at[:, q], a_buf.at[:, q], b_ssem.at[0, q], b_rsem.at[0, q], (me, q)
        )

    def pass_on(s, k, ssem, to):
        return remote(
            g_buf.at[s, k], g_buf.at[s, k], ssem.at[lax.div(s, 2), k], g_rsem.at[s, k], (to, tp)
        )

    def up(s, k):
        return pass_on(s, k, up_ssem, me + 2)

    def down(s, k):
        return pass_on(s, k, down_ssem, me - 2)

    def across(s, k):
        return pass_on(s, k, mate_ssem, mate)

    has_up = z < n_line - 1
    has_down = z > 0

    def send_own(k):
        load_g(k).wait()

        @pl.when(has_up)
        def _():
            up(me, k).start()

        @pl.when(has_down)
        def _():
            down(me, k).start()

        across(me, k).start()

    send_own(0)
    load_codes.wait()
    load_exps.wait()
    powers = jnp.exp2(exps_ref[...].astype(jnp.float32)).T
    for b in range(width // block):
        owner, place = divmod(b * block, feats)
        value = codes_ref[:, b * block : (b + 1) * block].astype(jnp.float32)
        value = value * powers[:, b : b + 1]
        a_send[owner, :, place : place + block] = value.astype(jnp.bfloat16)
    a_buf[me, tp] = a_send[me]
    for r in range(1, n_ctx):
        act_copy(lax.rem(me + r, n_ctx)).start()
    for k in range(1, CHUNKS):
        send_own(k)

    peers = [lax.rem(tp + r, n_tp) for r in range(1, n_tp)]
    if split:
        for q in peers:
            spread_copy(me, q, a_send.at[me]).start()
    for r in range(1, n_ctx):
        s = lax.rem(me + r, n_ctx)
        act_landing(s).wait_recv()
        if split:
            for q in peers:
                spread_copy(s, q).start()
    if not split:
        for q in peers:
            spread_all(q).start()

    grads = g_buf[me].reshape(-1, g_buf.shape[3])
    for i in range(n_d):
        load_w(i).wait()
        piece = lax.dot_general(
            grads, w_buf[i], (((1,), (1,)), ((), ())), preferred_element_type=jnp.float32
        ).astype(jnp.bfloat16)
        part[:, :, i * d_tile : (i + 1) * d_tile] = piece.reshape(n_tp, rows, d_tile)

    def part_copy(q):
        return remote(part.at[q], landed.at[tp], p_ssem.at[q], p_rsem.at[tp], (me, q))

    def part_landing(q):
        return remote(part.at[q], landed.at[q], p_ssem.at[q], p_rsem.at[q], (me, q))

    for q in peers:
        part_copy(q).start()

    n_cols = g_buf.shape[3]
    n_tile = 512 if n_cols % 512 == 0 else n_cols

    def accumulate(zz, first, k=None):
        if k is None:
            lhs = a_buf[pl.ds(2 * zz, 2)].reshape(-1, feats).T
        else:
            size = n_tp // CHUNKS
            lhs = a_buf[pl.ds(2 * zz, 2), k * size : (k + 1) * size].reshape(-1, feats).T

        for j in range(n_cols // n_tile):
            cols = slice(j * n_tile, (j + 1) * n_tile)
            if k is None:
                rhs = g_buf[pl.ds(2 * zz, 2), :, :, cols].reshape(-1, n_tile)
            else:
                rhs = g_buf[pl.ds(2 * zz, 2), k, :, cols].reshape(-1, n_tile)
            term = jnp.dot(lhs, rhs, preferred_element_type=jnp.float32) * scale
            if first:
                gw_ref[:, cols] = term
            else:
                gw_ref[:, cols] += term

    def await_acts(zz, first):
        if split:
            for c in range(2):
                for q in peers:
                    spread_landing(2 * zz + c, q).wait_recv()
        elif first:
            for q in peers:
                spread_all_landing(q).wait_recv()

    def chip_terms(zz, first=False):
        other = 2 * zz + 1 - core
        for k in range(CHUNKS):
            across(other, k).wait_recv()
        await_acts(zz, first)
        accumulate(zz, first)

    def terms_at(d):
        if d == 0:
            chip_terms(z, True)
            return

        @pl.when(z >= d)
        def _():
            chip_terms(z - d)

        @pl.when(z + d < n_line)
        def _():
            chip_terms(z + d)

    def sum_parts():
        for q in peers:
            part_landing(q).wait_recv()
        total = part[tp].astype(jnp.float32)
        for q in peers:
            total = total + landed[q].astype(jnp.float32)
        gin_ref[...] = total.astype(jnp.bfloat16)

    def from_below(d, k):
        s = me - 2 * d
        up(s, k).wait_recv()

        @pl.when(has_up)
        def _():
            up(s, k).start()

        across(s, k).start()

    def from_above(d, k):
        s = me + 2 * d
        down(s, k).wait_recv()

        @pl.when(has_down)
        def _():
            down(s, k).start()

        across(s, k).start()

    for d in range(1, n_line - 1):
        for k in range(CHUNKS):

            @pl.when(z >= d)
            def _():
                from_below(d, k)

            @pl.when(z + d < n_line)
            def _():
                from_above(d, k)

        terms_at(d - 1)

    d = n_line - 1
    terms_at(d - 1)

    def last_terms(zz, arrive):
        other = 2 * zz + 1 - core
        await_acts(zz, False)
        for k in range(CHUNKS):
            arrive(d, k)
            if k == CHUNKS - 1:
                sum_parts()
            if k > 0:
                across(other, k - 1).wait_recv()
                accumulate(zz, False, k - 1)
        across(other, CHUNKS - 1).wait_recv()
        accumulate(zz, False, CHUNKS - 1)

    @pl.when(z == d)
    def _():
        last_terms(0, from_below)

    @pl.when(z == 0)
    def _():
        last_terms(d, from_above)

    @pl.when((z > 0) & (z < d))
    def _():
        sum_parts()

    for r in range(1, n_ctx):
        act_copy(lax.rem(me + r, n_ctx)).wait_send()
    for q in peers:
        part_copy(q).wait_send()
        if split:
            for s in range(n_ctx):
                spread_copy(s, q).wait_send()
        else:
            spread_all(q).wait_send()
    for zz in range(n_line):
        for k in range(CHUNKS):
            s = 2 * zz + core
            across(s, k).wait_send()

            @pl.when(has_up & (zz <= z))
            def _():
                up(s, k).wait_send()

            @pl.when(has_down & (zz >= z))
            def _():
                down(s, k).wait_send()


def body(act_codes, scale_exps, weight, grad_out):
    n_ctx, n_tp = lax.axis_size("ctx"), lax.axis_size("tp")
    n_line = n_ctx // 2
    rows, width = act_codes.shape
    toks, cols = grad_out.shape
    feats = width // n_ctx
    d_tile = min(512, width)
    dma = pltpu.SemaphoreType.DMA
    vmem = pl.BlockSpec(memory_space=pltpu.VMEM)
    hbm = pl.BlockSpec(memory_space=pltpu.HBM)
    bf16 = jnp.bfloat16
    return pl.pallas_call(
        functools.partial(kernel, n_ctx, n_tp, toks * n_ctx),
        out_shape=(
            pltpu.VMEM((rows, width), bf16),
            pltpu.VMEM((feats, cols), jnp.float32),
        ),
        in_specs=[hbm, hbm, hbm, hbm],
        out_specs=(vmem, vmem),
        scratch_shapes=[
            pltpu.VMEM((rows, width), bf16),
            pltpu.VMEM(scale_exps.shape[::-1], scale_exps.dtype),
            pltpu.VMEM((width // d_tile, d_tile, cols), bf16),
            pltpu.VMEM((n_ctx, CHUNKS, toks // CHUNKS, cols), bf16),
            pltpu.VMEM((n_ctx, rows, feats), bf16),
            pltpu.VMEM((n_ctx, n_tp, rows, feats), bf16),
            pltpu.VMEM((n_tp, rows, width), bf16),
            pltpu.VMEM((n_tp, rows, width), bf16),
            dma((2,)),
            dma((width // d_tile,)),
            dma((CHUNKS,)),
            dma((n_ctx,)),
            dma((n_ctx,)),
            dma((n_ctx if n_ctx * n_tp <= 64 else 1, n_tp)),
            dma((n_ctx if n_ctx * n_tp <= 64 else 1, n_tp)),
            dma((n_line, CHUNKS)),
            dma((n_line, CHUNKS)),
            dma((n_line, CHUNKS)),
            dma((n_ctx, CHUNKS)),
            dma((n_tp,)),
            dma((n_tp,)),
        ],
        compiler_params=pltpu.CompilerParams(
            collective_id=0, has_side_effects=True, vmem_limit_bytes=40 * 1024 * 1024
        ),
    )(act_codes, scale_exps.T, weight, grad_out)


def solution(mesh):
    placed = (P(("ctx", "tp"), None), P(("ctx", "tp"), None), P(None, "tp"), P("ctx", "tp"))
    return jax.shard_map(
        body,
        mesh=mesh,
        in_specs=placed,
        out_specs=(P(("ctx", "tp"), None), P("ctx", "tp")),
        check_vma=False,
    )
```

```python
import functools

import jax
import jax.numpy as jnp
from jax import lax
from jax.experimental import pallas as pl
from jax.experimental.pallas import tpu as pltpu
from jax.sharding import PartitionSpec as P

MESH = pl.DeviceIdType.MESH
CHUNKS = 4


def kernel(
    n_ctx, n_tp, tokens,
    codes_hbm, exps_hbm, weight_ref, grads_ref,
    gin_ref, gw_ref,
    codes_ref, exps_ref, w_buf, g_buf, a_send, a_buf, part, landed,
    in_sem, w_sem, g_sem,
    a_ssem, a_rsem, b_ssem, b_rsem, up_ssem, down_ssem, mate_ssem, g_rsem, p_ssem, p_rsem,
):
    n_line = n_ctx // 2
    me = lax.axis_index("ctx")
    tp = lax.axis_index("tp")
    core = lax.rem(me, 2)
    z = lax.div(me, 2)
    mate = me + 1 - 2 * core
    rows, width = codes_ref.shape
    block = width // exps_ref.shape[0]
    feats = width // n_ctx
    d_tile = w_buf.shape[1]
    n_d = w_buf.shape[0]
    scale = lax.rsqrt(jnp.float32(tokens))
    split = n_ctx * n_tp <= 64

    def load_w(i):
        return pltpu.make_async_copy(
            weight_ref.at[pl.ds(i * d_tile, d_tile)], w_buf.at[i], w_sem.at[i]
        )

    def load_g(k):
        size = g_buf.shape[2]
        return pltpu.make_async_copy(
            grads_ref.at[pl.ds(k * size, size)], g_buf.at[me, k], g_sem.at[k]
        )

    load_codes = pltpu.make_async_copy(codes_hbm, codes_ref, in_sem.at[0])
    load_exps = pltpu.make_async_copy(exps_hbm, exps_ref, in_sem.at[1])
    load_g(0).start()
    load_codes.start()
    load_exps.start()
    for k in range(1, CHUNKS):
        load_g(k).start()
    for i in range(n_d):
        load_w(i).start()

    barrier = pltpu.get_barrier_semaphore()
    for r in range(1, n_ctx):
        pl.semaphore_signal(
            barrier, inc=1, device_id=(lax.rem(me + r, n_ctx), tp), device_id_type=MESH
        )
    for r in range(1, n_tp):
        pl.semaphore_signal(
            barrier, inc=1, device_id=(me, lax.rem(tp + r, n_tp)), device_id_type=MESH
        )

    pl.semaphore_wait(barrier, n_ctx + n_tp - 2)

    def remote(src, dst, ssem, rsem, to):
        return pltpu.make_async_remote_copy(
            src_ref=src, dst_ref=dst, send_sem=ssem, recv_sem=rsem,
            device_id=to, device_id_type=MESH,
        )

    def act_copy(to):
        return remote(
            a_send.at[to], a_buf.at[me, tp], a_ssem.at[to], a_rsem.at[me], (to, tp)
        )

    def act_landing(source):
        return remote(
            a_send.at[source], a_buf.at[source, tp], a_ssem.at[source], a_rsem.at[source],
            (source, tp),
        )

    def spread_copy(s, q, src=None):
        return remote(
            a_buf.at[s, tp] if src is None else src,
            a_buf.at[s, tp], b_ssem.at[s, q], b_rsem.at[s, tp], (me, q),
        )

    def spread_landing(s, q):
        return remote(
            a_buf.at[s, q], a_buf.at[s, q], b_ssem.at[s, q], b_rsem.at[s, q], (me, q)
        )

    def spread_all(q):
        return remote(
            a_buf.at[:, tp], a_buf.at[:, tp], b_ssem.at[0, q], b_rsem.at[0, tp], (me, q)
        )

    def spread_all_landing(q):
        return remote(
            a_buf.at[:, q], a_buf.at[:, q], b_ssem.at[0, q], b_rsem.at[0, q], (me, q)
        )

    def pass_on(s, k, ssem, to):
        return remote(
            g_buf.at[s, k], g_buf.at[s, k], ssem.at[lax.div(s, 2), k], g_rsem.at[s, k], (to, tp)
        )

    def up(s, k):
        return pass_on(s, k, up_ssem, me + 2)

    def down(s, k):
        return pass_on(s, k, down_ssem, me - 2)

    def across(s, k):
        return pass_on(s, k, mate_ssem, mate)

    has_up = z < n_line - 1
    has_down = z > 0

    def send_own(k):
        load_g(k).wait()

        @pl.when(has_up)
        def _():
            up(me, k).start()

        @pl.when(has_down)
        def _():
            down(me, k).start()

        across(me, k).start()

    send_own(0)
    load_codes.wait()
    load_exps.wait()
    powers = jnp.exp2(exps_ref[...].astype(jnp.float32)).T
    for b in range(width // block):
        owner, place = divmod(b * block, feats)
        value = codes_ref[:, b * block : (b + 1) * block].astype(jnp.float32)
        value = value * powers[:, b : b + 1]
        a_send[owner, :, place : place + block] = value.astype(jnp.bfloat16)
    a_buf[me, tp] = a_send[me]
    for r in range(1, n_ctx):
        act_copy(lax.rem(me + r, n_ctx)).start()
    for k in range(1, CHUNKS):
        send_own(k)

    peers = [lax.rem(tp + r, n_tp) for r in range(1, n_tp)]
    if split:
        for q in peers:
            spread_copy(me, q, a_send.at[me]).start()

    grads = g_buf.at[me]

    def part_piece(i):
        load_w(i).wait()
        rows_all = grads[...].reshape(-1, g_buf.shape[3])
        piece = lax.dot_general(
            rows_all, w_buf[i], (((1,), (1,)), ((), ())), preferred_element_type=jnp.float32
        ).astype(jnp.bfloat16)
        part[:, :, i * d_tile : (i + 1) * d_tile] = piece.reshape(n_tp, rows, d_tile)

    per = -(-n_d // n_ctx)
    done = 0
    for r in range(1, n_ctx):
        for i in range(done, min(done + per, n_d)):
            part_piece(i)
        done = min(done + per, n_d)
        s = lax.rem(me - r + n_ctx, n_ctx)
        act_landing(s).wait_recv()
        if split:
            for q in peers:
                spread_copy(s, q).start()
    for i in range(done, n_d):
        part_piece(i)
    if not split:
        for q in peers:
            spread_all(q).start()

    def part_copy(q):
        return remote(part.at[q], landed.at[tp], p_ssem.at[q], p_rsem.at[tp], (me, q))

    def part_landing(q):
        return remote(part.at[q], landed.at[q], p_ssem.at[q], p_rsem.at[q], (me, q))

    for q in peers:
        part_copy(q).start()

    n_cols = g_buf.shape[3]
    n_tile = 512 if n_cols % 512 == 0 else n_cols

    def accumulate(zz, first, k=None):
        if k is None:
            lhs = a_buf[pl.ds(2 * zz, 2)].reshape(-1, feats).T
        else:
            size = n_tp // CHUNKS
            lhs = a_buf[pl.ds(2 * zz, 2), k * size : (k + 1) * size].reshape(-1, feats).T

        for j in range(n_cols // n_tile):
            cols = slice(j * n_tile, (j + 1) * n_tile)
            if k is None:
                rhs = g_buf[pl.ds(2 * zz, 2), :, :, cols].reshape(-1, n_tile)
            else:
                rhs = g_buf[pl.ds(2 * zz, 2), k, :, cols].reshape(-1, n_tile)
            term = jnp.dot(lhs, rhs, preferred_element_type=jnp.float32) * scale
            if first:
                gw_ref[:, cols] = term
            else:
                gw_ref[:, cols] += term

    def await_acts(zz, first):
        if split:
            for c in range(2):
                for q in peers:
                    spread_landing(2 * zz + c, q).wait_recv()
        elif first:
            for q in peers:
                spread_all_landing(q).wait_recv()

    def chip_terms(zz, first=False):
        other = 2 * zz + 1 - core
        for k in range(CHUNKS):
            across(other, k).wait_recv()
        await_acts(zz, first)
        accumulate(zz, first)

    def terms_at(d):
        if d == 0:
            chip_terms(z, True)
            return

        @pl.when(z >= d)
        def _():
            chip_terms(z - d)

        @pl.when(z + d < n_line)
        def _():
            chip_terms(z + d)

    def sum_parts():
        for q in peers:
            part_landing(q).wait_recv()
        total = part[tp].astype(jnp.float32)
        for q in peers:
            total = total + landed[q].astype(jnp.float32)
        gin_ref[...] = total.astype(jnp.bfloat16)

    def from_below(d, k):
        s = me - 2 * d
        up(s, k).wait_recv()

        @pl.when(has_up)
        def _():
            up(s, k).start()

        across(s, k).start()

    def from_above(d, k):
        s = me + 2 * d
        down(s, k).wait_recv()

        @pl.when(has_down)
        def _():
            down(s, k).start()

        across(s, k).start()

    for d in range(1, n_line - 1):
        for k in range(CHUNKS):

            @pl.when(z >= d)
            def _():
                from_below(d, k)

            @pl.when(z + d < n_line)
            def _():
                from_above(d, k)

        terms_at(d - 1)

    d = n_line - 1
    terms_at(d - 1)

    def last_terms(zz, arrive):
        other = 2 * zz + 1 - core
        await_acts(zz, False)
        for k in range(CHUNKS):
            arrive(d, k)
            if k == CHUNKS - 1:
                sum_parts()
            if k > 0:
                across(other, k - 1).wait_recv()
                accumulate(zz, False, k - 1)
        across(other, CHUNKS - 1).wait_recv()
        accumulate(zz, False, CHUNKS - 1)

    @pl.when(z == d)
    def _():
        last_terms(0, from_below)

    @pl.when(z == 0)
    def _():
        last_terms(d, from_above)

    @pl.when((z > 0) & (z < d))
    def _():
        sum_parts()

    for r in range(1, n_ctx):
        act_copy(lax.rem(me + r, n_ctx)).wait_send()
    for q in peers:
        part_copy(q).wait_send()
        if split:
            for s in range(n_ctx):
                spread_copy(s, q).wait_send()
        else:
            spread_all(q).wait_send()
    for zz in range(n_line):
        for k in range(CHUNKS):
            s = 2 * zz + core
            across(s, k).wait_send()

            @pl.when(has_up & (zz <= z))
            def _():
                up(s, k).wait_send()

            @pl.when(has_down & (zz >= z))
            def _():
                down(s, k).wait_send()


def body(act_codes, scale_exps, weight, grad_out):
    n_ctx, n_tp = lax.axis_size("ctx"), lax.axis_size("tp")
    n_line = n_ctx // 2
    rows, width = act_codes.shape
    toks, cols = grad_out.shape
    feats = width // n_ctx
    d_tile = min(512, width)
    dma = pltpu.SemaphoreType.DMA
    lanes = -(-cols // 128) * 128
    outs = -(-rows // 16) * 16 * width * 2 + feats * lanes * 4
    vmem = pl.BlockSpec(memory_space=pltpu.VMEM)
    hbm = pl.BlockSpec(memory_space=pltpu.HBM)
    bf16 = jnp.bfloat16
    return pl.pallas_call(
        functools.partial(kernel, n_ctx, n_tp, toks * n_ctx),
        out_shape=(
            pltpu.VMEM((rows, width), bf16),
            pltpu.VMEM((feats, cols), jnp.float32),
        ),
        in_specs=[hbm, hbm, hbm, hbm],
        out_specs=(vmem, vmem),
        scratch_shapes=[
            pltpu.VMEM((rows, width), bf16),
            pltpu.VMEM(scale_exps.shape[::-1], scale_exps.dtype),
            pltpu.VMEM((width // d_tile, d_tile, cols), bf16),
            pltpu.VMEM((n_ctx, CHUNKS, toks // CHUNKS, cols), bf16),
            pltpu.VMEM((n_ctx, rows, feats), bf16),
            pltpu.VMEM((n_ctx, n_tp, rows, feats), bf16),
            pltpu.VMEM((n_tp, rows, width), bf16),
            pltpu.VMEM((n_tp, rows, width), bf16),
            dma((2,)),
            dma((width // d_tile,)),
            dma((CHUNKS,)),
            dma((n_ctx,)),
            dma((n_ctx,)),
            dma((n_ctx if n_ctx * n_tp <= 64 else 1, n_tp)),
            dma((n_ctx if n_ctx * n_tp <= 64 else 1, n_tp)),
            dma((n_line, CHUNKS)),
            dma((n_line, CHUNKS)),
            dma((n_line, CHUNKS)),
            dma((n_ctx, CHUNKS)),
            dma((n_tp,)),
            dma((n_tp,)),
        ],
        compiler_params=pltpu.CompilerParams(
            collective_id=0, has_side_effects=True, vmem_limit_bytes=67_043_328 - outs - 8192
        ),
    )(act_codes, scale_exps.T, weight, grad_out)


def solution(mesh):
    placed = (P(("ctx", "tp"), None), P(("ctx", "tp"), None), P(None, "tp"), P("ctx", "tp"))
    return jax.shard_map(
        body,
        mesh=mesh,
        in_specs=placed,
        out_specs=(P(("ctx", "tp"), None), P("ctx", "tp")),
        check_vma=False,
    )
```
